32 devices in a mesh: layer: 8 (over y, x, core), dp: 4 (over z).
Axes of the slice: x: 2, y: 2, z: 4, core: 2. Of those that a mesh axis runs over, the one named last changes fastest.
Arguments:
- initial: float32 [256, 1024], P('dp'), may hold values from -6 to 6
- norm_gains: float32 [32, 1024], P('layer'), may hold values from 0.25 to 1.75
- first_weights: bfloat16 [32, 1024, 2048], P('layer'), may hold values from -0.1875 to 0.1875
- second_weights: bfloat16 [32, 2048, 1024], P('layer'), may hold values from -0.046875 to 0.046875
Outputs:
- layer_states: float32 [32, 256, 1024], P('layer', 'dp')
- residual_ratios: float32 [7], replicated
- coarse_defects_four: float32 [32, 256, 1024], P('layer', 'dp')
- coarse_defects_sixteen: float32 [32, 256, 1024], P('layer', 'dp')
The draws below stay inside these ranges and needn't reach their ends.
All inputs are finite; a program needn't handle non-finite values.
Results may differ from the reference program's by a relative error of at most 0.02.
Values sent between devices are 32-bit elements; how exact they have to be, the bound alone decides.
A program may use at most 128 MiB of HBM per device.

```python
import jax
import jax.numpy as jnp
from jax import lax

D = 1024
FF = 2048
LAYERS = 32
TOKENS = 256


def steps_of(own_key, shape, cuts, least, high):
    level, own = 1.0, jax.random.fold_in(own_key, 6)
    for position, parts in cuts:
        steps = jnp.exp(jax.random.uniform(jax.random.fold_in(own, position), (parts,), jnp.float32, least / len(cuts), high / len(cuts)))
        level = level * jnp.repeat(steps, shape[position] // parts).reshape([-1 if axis == position else 1 for axis in range(len(shape))])
    return level


def noise(own_key, shape, scale, bound, cuts=(), kind=jnp.bfloat16):
    result = jax.random.normal(own_key, shape, jnp.float32) * scale
    if len(cuts) > 0:
        result = steps_of(own_key, shape, cuts, -0.22, 0.18) * result
    return jnp.clip(result, min=-bound, max=bound).astype(kind)


def setup_inputs(seed: int = 0) -> dict:
    key_of = jax.random.split(jax.random.key(seed), 5)
    initial = noise(key_of[0], (TOKENS, D), 1.0, 6.0, ((0, 4),), jnp.float32)
    norm_gains = jnp.clip(1.0 + 0.15 * jax.random.normal(key_of[1], (LAYERS, D), jnp.float32), 0.25, 1.75)
    first_weights = noise(key_of[2], (LAYERS, D, FF), D ** -0.5, 0.1875, ((0, 8),))
    second_weights = noise(key_of[3], (LAYERS, FF, D), (7 * FF) ** -0.5, 0.046875, ((0, 8),))
    return {"initial": initial, "norm_gains": norm_gains, "first_weights": first_weights, "second_weights": second_weights}


epsilon = 1e-06

def branch(row_block, weight_in, weight_out, gain_row):
    mean_square = lax.optimization_barrier(jnp.mean(row_block * row_block, axis=-1, keepdims=True))
    normed = (row_block * lax.rsqrt(mean_square + epsilon) * gain_row).astype(jnp.bfloat16)
    hidden = jax.nn.gelu(jnp.dot(normed, weight_in, preferred_element_type=jnp.float32), approximate=True).astype(jnp.bfloat16)
    return jnp.dot(hidden, weight_out, preferred_element_type=jnp.float32)

def reference(initial, norm_gains, first_weights, second_weights):
    layer_total = LAYERS
    history = [initial] * (layer_total + 1)

    def propagate(point, values, spacing):
        return values + spacing * branch(values, first_weights[point - 1], second_weights[point - 1], norm_gains[point - 1])

    def relaxation(spacing, residues, right_side):
        for residue in residues:
            for point in range(spacing, layer_total + 1, spacing):
                if point % (4 * spacing) == residue:
                    updated = propagate(point, history[point - spacing], spacing)
                    if right_side is not None:
                        updated = updated + right_side[point]
                    history[point] = updated

    def restrict(spacing, right_side):
        coarse = {}
        gap_sums = []
        step_sums = []
        for point in range(4 * spacing, layer_total + 1, 4 * spacing):
            before = history[point - spacing]
            update = branch(before, first_weights[point - 1], second_weights[point - 1], norm_gains[point - 1])
            fine_value = before + spacing * update
            if right_side is not None:
                fine_value = fine_value + right_side[point]
            coarse[point] = fine_value - propagate(point, history[point - 4 * spacing], 4 * spacing)
            gap = fine_value - history[point]
            gap_sums.append(jnp.sum(gap * gap))
            step_sums.append(jnp.sum(update * update))
        return (coarse, gap_sums, step_sums)

    def defects(spacing):
        rows = []
        for point in range(1, layer_total + 1):
            if point >= spacing:
                rows.append(history[point] - propagate(point, history[point - spacing], spacing))
            else:
                rows.append(jnp.zeros_like(initial))
        return jnp.stack(rows)
    relaxation(1, (1, 2, 3), None)
    relaxation(1, (0,), None)
    relaxation(1, (1, 2, 3), None)
    rhs_one, gap_sums, step_sums = restrict(1, None)
    relaxation(4, (4, 8, 12), rhs_one)
    rhs_two, unused_gaps, unused_steps = restrict(4, rhs_one)
    for point in range(16, layer_total + 1, 16):
        history[point] = propagate(point, history[point - 16], 16) + rhs_two[point]
    relaxation(4, (4, 8, 12), rhs_one)
    relaxation(1, (1, 2, 3), None)
    layer_states = jnp.stack(history[1:])
    residual_ratios = jnp.sqrt(jnp.stack(gap_sums[1:]) / (jnp.stack(step_sums[1:]) + epsilon))
    defects_four = defects(4)
    defects_sixteen = defects(16)
    return (layer_states, residual_ratios, defects_four, defects_sixteen)
```

```python
import jax
import jax.numpy as jnp
from jax import lax
from jax.experimental import pallas as pl
from jax.experimental.pallas import tpu as pltpu
from jax.sharding import PartitionSpec as P

epsilon = 1e-06


def shifted(block, axis, distance):
    devices = range(lax.axis_size(axis))
    route = [(i - distance, i) for i in devices if i - distance in devices]
    return lax.ppermute(block, axis, route)


def branch(row_block, weight_in, weight_out, gain_row):
    mean_square = jnp.mean(row_block * row_block, axis=-1, keepdims=True)
    normed = (row_block * lax.rsqrt(mean_square + epsilon) * gain_row).astype(jnp.bfloat16)
    hidden = jax.nn.gelu(
        jnp.dot(normed, weight_in, preferred_element_type=jnp.float32), approximate=True
    ).astype(jnp.bfloat16)
    return jnp.dot(hidden, weight_out, preferred_element_type=jnp.float32)


def local(initial, norm_gains, first_weights, second_weights):
    slot_count = first_weights.shape[0]
    sections = lax.axis_size("layer")
    layer_total = slot_count * sections
    norm_count = layer_total // 4 - 1
    first_point = lax.axis_index("layer") * slot_count
    points = first_point + jnp.arange(slot_count, dtype=jnp.int32) + 1
    spacings = (1, 4, 16)

    def shaped(flags, rank):
        return flags.reshape((slot_count,) + (1,) * (rank - 1))

    def previous(values, level_index):
        spacing = spacings[level_index]
        if spacing >= slot_count:
            portion = values
            distance = spacing // slot_count
        else:
            portion = values[slot_count - spacing :]
            distance = 1
        if level_index == 0:
            arrived = shifted(portion, "layer", distance)
        elif level_index == 1:
            arrived = shifted(portion, "layer", distance)
        else:
            arrived = shifted(portion, "layer", distance)
        if spacing < slot_count:
            arrived = jnp.concatenate([arrived, values[: slot_count - spacing]], axis=0)
        return arrived

    def incoming(values, level_index, anchor):
        arrived = previous(values, level_index)
        from_anchor = shaped(points - spacings[level_index] == 0, values.ndim)
        return jnp.where(from_anchor, anchor, arrived)

    def advance(before, level_index, active, right_side):
        factor = float(spacings[level_index])
        results = []
        for slot in range(slot_count):

            def advance_compute(values, source, slot=slot):
                return (
                    values
                    + factor
                    * branch(values, first_weights[slot], second_weights[slot], norm_gains[slot])
                    + source
                )

            def advance_unchanged(values, source):
                return values

            source = right_side[slot] if right_side is not None else jnp.zeros_like(before[slot])
            results.append(
                lax.cond(active[slot], advance_compute, advance_unchanged, before[slot], source)
            )
        return jnp.stack(results)

    def relaxation(current, level_index, residues, right_side, anchor):
        modulus = 4 * spacings[level_index]
        for residue in residues:
            before = incoming(current, level_index, anchor)
            active = points % modulus == residue
            current = jnp.where(
                shaped(active, 3), advance(before, level_index, active, right_side), current
            )
        return (current, None)

    def restrict(current, level_index, right_side, anchor):
        spacing = spacings[level_index]
        factor = float(spacing)
        wide_factor = float(4 * spacing)
        before = incoming(current, level_index, anchor)
        far_state = incoming(current, level_index + 1, anchor)
        active = points % (4 * spacing) == 0
        row_count = current.shape[1]
        coarse_list = []
        gap_list = []
        step_list = []
        for slot in range(slot_count):

            def restrict_compute(near, distant, held, source, slot=slot):
                update = branch(
                    jnp.concatenate([near, distant], axis=0),
                    first_weights[slot],
                    second_weights[slot],
                    norm_gains[slot],
                )
                near_term = update[:row_count]
                fine_value = near + factor * near_term + source
                coarse = fine_value - (distant + wide_factor * update[row_count:])
                gap = fine_value - held
                return (coarse, jnp.sum(gap * gap), jnp.sum(near_term * near_term))

            def restrict_unchanged(near, distant, held, source):
                nothing = jnp.zeros((), near.dtype)
                return (jnp.zeros_like(near), nothing, nothing)

            source = right_side[slot] if right_side is not None else jnp.zeros_like(before[slot])
            coarse, gap_sum, step_sum = lax.cond(
                active[slot],
                restrict_compute,
                restrict_unchanged,
                before[slot],
                far_state[slot],
                current[slot],
                source,
            )
            coarse_list.append(coarse)
            gap_list.append(gap_sum)
            step_list.append(step_sum)
        return (jnp.stack(coarse_list), jnp.stack(gap_list), jnp.stack(step_list))

    def defects(current, level_index, anchor):
        spacing = spacings[level_index]
        factor = float(spacing)
        before = incoming(current, level_index, anchor)
        stepped = []
        for slot in range(slot_count):
            stepped.append(
                before[slot]
                + factor
                * branch(before[slot], first_weights[slot], second_weights[slot], norm_gains[slot])
            )
        valid = shaped(points >= spacing, 3)
        return jnp.where(valid, current - jnp.stack(stepped), 0.0)

    def multigrid_cycle(anchor):
        current = jnp.broadcast_to(anchor, (slot_count,) + anchor.shape)
        current, unused = relaxation(current, 0, (1, 2, 3), None, anchor)
        current, unused = relaxation(current, 0, (0,), None, anchor)
        current, carried = relaxation(current, 0, (1, 2, 3), None, anchor)
        rhs_one, gap_sums, step_sums = restrict(current, 0, None, anchor)
        current, carried = relaxation(current, 1, (4, 8, 12), rhs_one, anchor)
        rhs_two, unused_gaps, unused_steps = restrict(current, 1, rhs_one, anchor)
        for coarse_step in range(1, layer_total // 16 + 1):
            active = points == 16 * coarse_step
            before = incoming(current, 2, anchor)
            current = jnp.where(shaped(active, 3), advance(before, 2, active, rhs_two), current)
        current, unused = relaxation(current, 1, (4, 8, 12), rhs_one, anchor)
        current, unused = relaxation(current, 0, (1, 2, 3), None, anchor)
        defects_four = defects(current, 1, anchor)
        defects_sixteen = defects(current, 2, anchor)
        return (current, gap_sums, step_sums, defects_four, defects_sixteen)

    portions = [initial]
    outcomes = [multigrid_cycle(portion) for portion in portions]
    layer_states = jnp.concatenate([outcome[0] for outcome in outcomes], axis=1)
    defects_four = jnp.concatenate([outcome[3] for outcome in outcomes], axis=1)
    defects_sixteen = jnp.concatenate([outcome[4] for outcome in outcomes], axis=1)
    gap_sums = outcomes[0][1]
    step_sums = outcomes[0][2]
    counted = (points % 4 == 0) & (points >= 8)
    entry_index = points // 4 - 2
    one_hot = (
        (jnp.arange(norm_count, dtype=jnp.int32)[None, :] == entry_index[:, None])
        & counted[:, None]
    ).astype(jnp.float32)
    gap_vector = jnp.sum(gap_sums[:, None] * one_hot, axis=0)
    step_vector = jnp.sum(step_sums[:, None] * one_hot, axis=0)
    gap_total, step_total = lax.psum((gap_vector, step_vector), ("layer", "dp"))
    residual_ratios = jnp.sqrt(gap_total / (step_total + epsilon))
    return (layer_states, residual_ratios, defects_four, defects_sixteen)


def cycle_kernel(
    sections, copies,
    initial, norm_gains, first_weights, second_weights,
    out_states, out_four, out_sixteen, ratios,
    w_in, w_out, gain, start, normed, hidden, total, cur,
    relaxed, middle, final, rhs, wide_start,
    left_relaxed, left_middle, left_final, far_relaxed, far_final, lefts, fars,
    states, four, sixteen, tile, across, along, summed,
    load_in, load_out, load_small, store,
    send_point, take_point, send_state, take_state,
    across_send, across_take, along_send, along_take,
):
    here = lax.axis_index("layer")
    depth = lax.axis_index("dp")
    slot_count, width, ff = w_in.shape
    rows = start.shape[0]
    half = sections // 2
    end = sections - 1
    slot_last = slot_count - 1

    def to(layer, dp):
        return dict(device_id=(layer, dp), device_id_type=pl.DeviceIdType.MESH)

    def load_first(slot):
        return pltpu.make_async_copy(first_weights.at[slot], w_in.at[slot], load_in.at[slot])

    def load_second(slot):
        return pltpu.make_async_copy(second_weights.at[slot], w_out.at[slot], load_out.at[slot])

    load_start = pltpu.make_async_copy(initial, start, load_small.at[0])
    load_gain = pltpu.make_async_copy(norm_gains, gain, load_small.at[1])
    load_start.start()
    load_gain.start()
    for slot in range(slot_count):
        load_first(slot).start()
        load_second(slot).start()

    barrier = pltpu.get_barrier_semaphore()
    for k in range(1, sections):
        pl.semaphore_signal(barrier, inc=1, **to(lax.rem(here + k, sections), depth))
    for k in range(1, copies):
        pl.semaphore_signal(barrier, inc=1, **to(here, lax.rem(depth + k, copies)))

    def point_send(kind, source, target, distance):
        return pltpu.make_async_remote_copy(
            src_ref=source, dst_ref=target,
            send_sem=send_point.at[kind], recv_sem=take_point.at[kind],
            **to(lax.rem(here + distance, sections), depth),
        )

    give_relaxed = point_send(0, relaxed, left_relaxed, 1)
    give_far_relaxed = point_send(1, relaxed, far_relaxed, half)
    give_middle = point_send(2, middle, left_middle, 1)
    give_final = point_send(3, final, left_final, 1)
    give_far_final = point_send(4, final, far_final, half)

    def state_send(slot, target, distance, row):
        return pltpu.make_async_remote_copy(
            src_ref=states.at[slot], dst_ref=target.at[slot],
            send_sem=send_state.at[row, slot], recv_sem=take_state.at[row, slot],
            **to(lax.rem(here + distance, sections), depth),
        )

    def give_left(slot):
        return state_send(slot, lefts, 1, 0)

    def give_far(slot):
        return state_send(slot, fars, half, 1)

    def across_copy(k):
        return pltpu.make_async_remote_copy(
            src_ref=tile, dst_ref=across.at[depth],
            send_sem=across_send.at[k - 1], recv_sem=across_take.at[k - 1],
            **to(here, lax.rem(depth + k, copies)),
        )

    def along_copy(k):
        return pltpu.make_async_remote_copy(
            src_ref=summed, dst_ref=along.at[k - 1],
            send_sem=along_send.at[k - 1], recv_sem=along_take.at[k - 1],
            **to(lax.rem(here + k, sections), depth),
        )

    def normalise(part, values, slot):
        mean_square = jnp.mean(values * values, axis=-1, keepdims=True)
        normed[part * rows : (part + 1) * rows, :] = (
            values * lax.rsqrt(mean_square + epsilon) * gain[pl.ds(slot, 1), :]
        ).astype(jnp.bfloat16)

    def project_in(parts, slot):
        step = ff // 4
        for i in range(4):
            cols = slice(i * step, (i + 1) * step)
            hidden[: parts * rows, cols] = jax.nn.gelu(
                jnp.dot(
                    normed[: parts * rows, :], w_in[slot, :, cols],
                    preferred_element_type=jnp.float32,
                ),
                approximate=True,
            ).astype(jnp.bfloat16)

    def project_out(parts, slot):
        step = width // 4
        for i in range(4):
            cols = slice(i * step, (i + 1) * step)
            total[: parts * rows, cols] = jnp.dot(
                hidden[: parts * rows, :], w_out[slot, :, cols],
                preferred_element_type=jnp.float32,
            )

    def update(part):
        return total[part * rows : (part + 1) * rows, :]

    load_start.wait()
    load_gain.wait()
    cur[...] = start[...]

    def first_pass(slot, carry):
        normalise(0, cur[...], slot)
        normalise(1, start[...], slot)
        load_first(slot).wait()
        project_in(2, slot)
        load_second(slot).wait()
        project_out(2, slot)
        state = cur[...] + update(0)
        cur[...] = state
        states[slot] = state
        return carry

    lax.fori_loop(0, slot_count, first_pass, 0)
    relaxed[...] = cur[...]
    pl.semaphore_wait(barrier, sections + copies - 2)

    @pl.when(here < end)
    def _():
        give_relaxed.start()

    @pl.when(here == half - 1)
    def _():
        give_far_relaxed.start()

    four[...] = jnp.zeros_like(four)
    sixteen[...] = jnp.zeros_like(sixteen)
    tile[...] = jnp.zeros_like(tile)

    @pl.when(here == half - 1)
    def _():
        wide_start[...] = start[...] + 16.0 * update(1)

    @pl.when(here == 0)
    def _():
        final[...] = relaxed[...]
        give_far_final.start()
        four[slot_last] = relaxed[...] - (start[...] + 4.0 * update(1))
        for slot in range(slot_last):
            give_left(slot).start()
            give_far(slot).start()

    @pl.when(here > 0)
    def _():
        give_relaxed.wait_recv()
        cur[...] = left_relaxed[...]

        def second_pass(slot, carry):
            normalise(0, cur[...], slot)

            @pl.when(slot == slot_last)
            def _():
                normalise(1, left_relaxed[...], slot)

            project_in(2, slot)
            project_out(2, slot)
            state = cur[...] + update(0)
            cur[...] = state
            states[slot] = state
            return carry

        lax.fori_loop(0, slot_count, second_pass, 0)

        @pl.when(here == 1)
        def _():
            final[...] = cur[...]
            give_final.start()
            give_far_final.start()
            for slot in range(slot_last):
                give_left(slot).start()
                give_far(slot).start()

        @pl.when(here == half)
        def _():
            middle[...] = cur[...]
            give_middle.start()

        fine = cur[...]
        source = fine - (left_relaxed[...] + 4.0 * update(1))
        rhs[...] = source

        @pl.when(here == 1)
        def _():
            four[slot_last] = source

        gap = fine - relaxed[...]
        near_term = update(0)
        lane = lax.broadcasted_iota(jnp.int32, tile.shape, 1) == here - 1
        row = lax.broadcasted_iota(jnp.int32, tile.shape, 0)
        tile[...] = jnp.where(lane & (row == 0), jnp.sum(gap * gap), 0.0) + jnp.where(
            lane & (row == 1), jnp.sum(near_term * near_term), 0.0
        )

    across[depth] = tile[...]
    for k in range(1, copies):
        across_copy(k).start()

    def coarse_pass(r, carry):
        middle_round = (r == 0) & (here > half)
        wide_round = (r == 1) & (here == end)
        final_round = (r == 2) & (here > 1)

        @pl.when(middle_round | wide_round | final_round)
        def _():
            @pl.when(middle_round)
            def _():
                give_middle.wait_recv()
                normalise(0, left_middle[...], slot_last)

            @pl.when(wide_round)
            def _():
                give_far_relaxed.wait_recv()
                normalise(1, far_relaxed[...], slot_last)
                give_far_final.wait_recv()
                normalise(0, far_final[...], slot_last)

            @pl.when(final_round)
            def _():
                @pl.when((here >= half) & (here < end))
                def _():
                    give_far_final.wait_recv()
                    normalise(1, far_final[...], slot_last)

                give_final.wait_recv()
                normalise(0, left_final[...], slot_last)

            project_in(2, slot_last)
            project_out(2, slot_last)

            @pl.when(middle_round)
            def _():
                middle[...] = left_middle[...] + 4.0 * update(0) + rhs[...]

                @pl.when(here < end)
                def _():
                    give_middle.start()

            @pl.when(wide_round)
            def _():
                stepped = far_final[...] + 16.0 * update(0)
                point = stepped + (middle[...] - (far_relaxed[...] + 16.0 * update(1)))
                final[...] = point
                sixteen[slot_last] = point - stepped

            @pl.when(final_round)
            def _():
                stepped = left_final[...] + 4.0 * update(0)

                @pl.when(here < end)
                def _():
                    final[...] = stepped + rhs[...]
                    give_final.start()

                @pl.when(here < half)
                def _():
                    give_far_final.start()

                point = final[...]
                four[slot_last] = point - stepped

                @pl.when(here == half - 1)
                def _():
                    sixteen[slot_last] = point - wide_start[...]

                @pl.when((here >= half) & (here < end))
                def _():
                    sixteen[slot_last] = point - (far_final[...] + 16.0 * update(1))

        return carry

    lax.fori_loop(0, 3, coarse_pass, 0)

    for k in range(1, copies):
        across_copy(k).wait()
    gathered = across[0]
    for k in range(1, copies):
        gathered = gathered + across[k]
    summed[...] = gathered
    for k in range(1, sections):
        along_copy(k).start()

    states[slot_last] = final[...]

    @pl.when(here > 0)
    def _():
        @pl.when(here > 1)
        def _():
            cur[...] = left_final[...]

        def last_pass(slot, carry):
            @pl.when(here > 1)
            def _():
                normalise(0, cur[...], slot)

            give_left(slot).wait_recv()
            normalise(1, lefts[slot], slot)

            @pl.when(here >= half)
            def _():
                give_far(slot).wait_recv()
                normalise(2, fars[slot], slot)

            project_in(3, slot)
            project_out(3, slot)

            @pl.when(here > 1)
            def _():
                state = cur[...] + update(0)
                cur[...] = state
                states[slot] = state

                @pl.when(here < end)
                def _():
                    give_left(slot).start()

                @pl.when(here < half)
                def _():
                    give_far(slot).start()

            state = states[slot]
            four[slot] = state - (lefts[slot] + 4.0 * update(1))

            @pl.when(here >= half)
            def _():
                sixteen[slot] = state - (fars[slot] + 16.0 * update(2))

            return carry

        lax.fori_loop(0, slot_last, last_pass, 0)

    results = (
        pltpu.make_async_copy(states, out_states, store.at[0]),
        pltpu.make_async_copy(four, out_four, store.at[1]),
        pltpu.make_async_copy(sixteen, out_sixteen, store.at[2]),
    )
    for copy in results:
        copy.start()

    @pl.when(here < end)
    def _():
        give_relaxed.wait_send()
        for slot in range(slot_last):
            give_left(slot).wait_send()

    @pl.when(here == half - 1)
    def _():
        give_far_relaxed.wait_send()

    @pl.when((here >= half) & (here < end))
    def _():
        give_middle.wait_send()

    @pl.when((here > 0) & (here < end))
    def _():
        give_final.wait_send()

    @pl.when(here < half)
    def _():
        give_far_final.wait_send()
        for slot in range(slot_last):
            give_far(slot).wait_send()

    sums = summed[...]
    for k in range(1, sections):
        along_copy(k).wait()
        sums = sums + along[k - 1]
    ratios[...] = jnp.sqrt(sums[0:1] / (sums[1:2] + epsilon))
    for copy in results:
        copy.wait()


def cycle(initial, norm_gains, first_weights, second_weights):
    sections = lax.axis_size("layer")
    copies = lax.axis_size("dp")
    shape = initial.shape
    slot_count, width, ff = first_weights.shape
    rows = shape[0]
    anywhere = pl.BlockSpec(memory_space=pl.ANY)
    held = (slot_count,) + shape
    inner = (slot_count - 1,) + shape
    dma = pltpu.SemaphoreType.DMA

    def single(*dims):
        return pltpu.VMEM(dims, jnp.float32)

    states, four, sixteen, ratios = pl.pallas_call(
        lambda *refs: cycle_kernel(sections, copies, *refs),
        out_shape=(
            jax.ShapeDtypeStruct(held, jnp.float32),
            jax.ShapeDtypeStruct(held, jnp.float32),
            jax.ShapeDtypeStruct(held, jnp.float32),
            jax.ShapeDtypeStruct((1, 128), jnp.float32),
        ),
        in_specs=[anywhere] * 4,
        out_specs=(anywhere, anywhere, anywhere, pl.BlockSpec(memory_space=pltpu.VMEM)),
        scratch_shapes=[
            pltpu.VMEM(first_weights.shape, jnp.bfloat16),
            pltpu.VMEM(second_weights.shape, jnp.bfloat16),
            single(slot_count, width),
            single(*shape),
            pltpu.VMEM((3 * rows, width), jnp.bfloat16),
            pltpu.VMEM((3 * rows, ff), jnp.bfloat16),
            single(3 * rows, width),
            single(*shape),
            single(*shape), single(*shape), single(*shape), single(*shape), single(*shape),
            single(*shape), single(*shape), single(*shape), single(*shape), single(*shape),
            single(*inner), single(*inner),
            single(*held), single(*held), single(*held),
            single(8, 128), single(copies, 8, 128), single(sections - 1, 8, 128), single(8, 128),
            dma((slot_count,)), dma((slot_count,)), dma((2,)), dma((3,)),
            dma((5,)), dma((5,)), dma((2, slot_count - 1)), dma((2, slot_count - 1)),
            dma((copies - 1,)), dma((copies - 1,)),
            dma((sections - 1,)), dma((sections - 1,)),
        ],
        compiler_params=pltpu.CompilerParams(
            collective_id=0, has_side_effects=True, vmem_limit_bytes=60 * 1024 * 1024
        ),
        name="cycle",
    )(initial, norm_gains, first_weights, second_weights)
    return (states, ratios[0, : sections - 1], four, sixteen)


def chosen(initial, norm_gains, first_weights, second_weights):
    sections = lax.axis_size("layer")
    fits = first_weights.shape[0] == 4 and sections == 8 and lax.axis_size("dp") > 1
    return (cycle if fits else local)(initial, norm_gains, first_weights, second_weights)


def solution(mesh):
    placed = (P("dp", None), P("layer", None), P("layer", None, None), P("layer", None, None))
    return jax.shard_map(
        chosen,
        mesh=mesh,
        in_specs=placed,
        out_specs=(P("layer", "dp", None), P(), P("layer", "dp", None), P("layer", "dp", None)),
        check_vma=False,
    )
```

```python
import jax
import jax.numpy as jnp
from jax import lax
from jax.experimental import pallas as pl
from jax.experimental.pallas import tpu as pltpu
from jax.sharding import PartitionSpec as P

epsilon = 1e-06


def shifted(block, axis, distance):
    devices = range(lax.axis_size(axis))
    route = [(i - distance, i) for i in devices if i - distance in devices]
    return lax.ppermute(block, axis, route)


def branch(row_block, weight_in, weight_out, gain_row):
    mean_square = jnp.mean(row_block * row_block, axis=-1, keepdims=True)
    normed = (row_block * lax.rsqrt(mean_square + epsilon) * gain_row).astype(jnp.bfloat16)
    hidden = jax.nn.gelu(
        jnp.dot(normed, weight_in, preferred_element_type=jnp.float32), approximate=True
    ).astype(jnp.bfloat16)
    return jnp.dot(hidden, weight_out, preferred_element_type=jnp.float32)


def local(initial, norm_gains, first_weights, second_weights):
    slot_count = first_weights.shape[0]
    sections = lax.axis_size("layer")
    layer_total = slot_count * sections
    norm_count = layer_total // 4 - 1
    first_point = lax.axis_index("layer") * slot_count
    points = first_point + jnp.arange(slot_count, dtype=jnp.int32) + 1
    spacings = (1, 4, 16)

    def shaped(flags, rank):
        return flags.reshape((slot_count,) + (1,) * (rank - 1))

    def previous(values, level_index):
        spacing = spacings[level_index]
        if spacing >= slot_count:
            portion = values
            distance = spacing // slot_count
        else:
            portion = values[slot_count - spacing :]
            distance = 1
        if level_index == 0:
            arrived = shifted(portion, "layer", distance)
        elif level_index == 1:
            arrived = shifted(portion, "layer", distance)
        else:
            arrived = shifted(portion, "layer", distance)
        if spacing < slot_count:
            arrived = jnp.concatenate([arrived, values[: slot_count - spacing]], axis=0)
        return arrived

    def incoming(values, level_index, anchor):
        arrived = previous(values, level_index)
        from_anchor = shaped(points - spacings[level_index] == 0, values.ndim)
        return jnp.where(from_anchor, anchor, arrived)

    def advance(before, level_index, active, right_side):
        factor = float(spacings[level_index])
        results = []
        for slot in range(slot_count):

            def advance_compute(values, source, slot=slot):
                return (
                    values
                    + factor
                    * branch(values, first_weights[slot], second_weights[slot], norm_gains[slot])
                    + source
                )

            def advance_unchanged(values, source):
                return values

            source = right_side[slot] if right_side is not None else jnp.zeros_like(before[slot])
            results.append(
                lax.cond(active[slot], advance_compute, advance_unchanged, before[slot], source)
            )
        return jnp.stack(results)

    def relaxation(current, level_index, residues, right_side, anchor):
        modulus = 4 * spacings[level_index]
        for residue in residues:
            before = incoming(current, level_index, anchor)
            active = points % modulus == residue
            current = jnp.where(
                shaped(active, 3), advance(before, level_index, active, right_side), current
            )
        return (current, None)

    def restrict(current, level_index, right_side, anchor):
        spacing = spacings[level_index]
        factor = float(spacing)
        wide_factor = float(4 * spacing)
        before = incoming(current, level_index, anchor)
        far_state = incoming(current, level_index + 1, anchor)
        active = points % (4 * spacing) == 0
        row_count = current.shape[1]
        coarse_list = []
        gap_list = []
        step_list = []
        for slot in range(slot_count):

            def restrict_compute(near, distant, held, source, slot=slot):
                update = branch(
                    jnp.concatenate([near, distant], axis=0),
                    first_weights[slot],
                    second_weights[slot],
                    norm_gains[slot],
                )
                near_term = update[:row_count]
                fine_value = near + factor * near_term + source
                coarse = fine_value - (distant + wide_factor * update[row_count:])
                gap = fine_value - held
                return (coarse, jnp.sum(gap * gap), jnp.sum(near_term * near_term))

            def restrict_unchanged(near, distant, held, source):
                nothing = jnp.zeros((), near.dtype)
                return (jnp.zeros_like(near), nothing, nothing)

            source = right_side[slot] if right_side is not None else jnp.zeros_like(before[slot])
            coarse, gap_sum, step_sum = lax.cond(
                active[slot],
                restrict_compute,
                restrict_unchanged,
                before[slot],
                far_state[slot],
                current[slot],
                source,
            )
            coarse_list.append(coarse)
            gap_list.append(gap_sum)
            step_list.append(step_sum)
        return (jnp.stack(coarse_list), jnp.stack(gap_list), jnp.stack(step_list))

    def defects(current, level_index, anchor):
        spacing = spacings[level_index]
        factor = float(spacing)
        before = incoming(current, level_index, anchor)
        stepped = []
        for slot in range(slot_count):
            stepped.append(
                before[slot]
                + factor
                * branch(before[slot], first_weights[slot], second_weights[slot], norm_gains[slot])
            )
        valid = shaped(points >= spacing, 3)
        return jnp.where(valid, current - jnp.stack(stepped), 0.0)

    def multigrid_cycle(anchor):
        current = jnp.broadcast_to(anchor, (slot_count,) + anchor.shape)
        current, unused = relaxation(current, 0, (1, 2, 3), None, anchor)
        current, unused = relaxation(current, 0, (0,), None, anchor)
        current, carried = relaxation(current, 0, (1, 2, 3), None, anchor)
        rhs_one, gap_sums, step_sums = restrict(current, 0, None, anchor)
        current, carried = relaxation(current, 1, (4, 8, 12), rhs_one, anchor)
        rhs_two, unused_gaps, unused_steps = restrict(current, 1, rhs_one, anchor)
        for coarse_step in range(1, layer_total // 16 + 1):
            active = points == 16 * coarse_step
            before = incoming(current, 2, anchor)
            current = jnp.where(shaped(active, 3), advance(before, 2, active, rhs_two), current)
        current, unused = relaxation(current, 1, (4, 8, 12), rhs_one, anchor)
        current, unused = relaxation(current, 0, (1, 2, 3), None, anchor)
        defects_four = defects(current, 1, anchor)
        defects_sixteen = defects(current, 2, anchor)
        return (current, gap_sums, step_sums, defects_four, defects_sixteen)

    portions = [initial]
    outcomes = [multigrid_cycle(portion) for portion in portions]
    layer_states = jnp.concatenate([outcome[0] for outcome in outcomes], axis=1)
    defects_four = jnp.concatenate([outcome[3] for outcome in outcomes], axis=1)
    defects_sixteen = jnp.concatenate([outcome[4] for outcome in outcomes], axis=1)
    gap_sums = outcomes[0][1]
    step_sums = outcomes[0][2]
    counted = (points % 4 == 0) & (points >= 8)
    entry_index = points // 4 - 2
    one_hot = (
        (jnp.arange(norm_count, dtype=jnp.int32)[None, :] == entry_index[:, None])
        & counted[:, None]
    ).astype(jnp.float32)
    gap_vector = jnp.sum(gap_sums[:, None] * one_hot, axis=0)
    step_vector = jnp.sum(step_sums[:, None] * one_hot, axis=0)
    gap_total, step_total = lax.psum((gap_vector, step_vector), ("layer", "dp"))
    residual_ratios = jnp.sqrt(gap_total / (step_total + epsilon))
    return (layer_states, residual_ratios, defects_four, defects_sixteen)


def cycle_kernel(
    sections, copies,
    initial, norm_gains, first_weights, second_weights,
    states, four, sixteen, ratios,
    w_in, w_out, gain, start, normed, hidden, total, cur,
    relaxed, middle, final, rhs, wide_start,
    fine, near, left_relaxed, left_middle, left_final, far_relaxed, far_final, lefts, fars,
    tile, across, along, summed,
    load_in, load_out, load_small,
    send_point, take_point, send_state, take_state,
    across_send, across_take, along_send, along_take,
):
    here = lax.axis_index("layer")
    depth = lax.axis_index("dp")
    slot_count, width, ff = w_in.shape
    rows = start.shape[0]
    half = sections // 2
    end = sections - 1
    slot_last = slot_count - 1

    def to(layer, dp):
        return dict(device_id=(layer, dp), device_id_type=pl.DeviceIdType.MESH)

    def load_first(slot):
        return pltpu.make_async_copy(first_weights.at[slot], w_in.at[slot], load_in.at[slot])

    def load_second(slot):
        return pltpu.make_async_copy(second_weights.at[slot], w_out.at[slot], load_out.at[slot])

    load_start = pltpu.make_async_copy(initial, start, load_small.at[0])
    load_gain = pltpu.make_async_copy(norm_gains, gain, load_small.at[1])
    load_start.start()
    load_gain.start()
    ahead = min(2, slot_count)
    for slot in range(ahead):
        load_first(slot).start()
        load_second(slot).start()

    barrier = pltpu.get_barrier_semaphore()
    for k in range(1, sections):
        pl.semaphore_signal(barrier, inc=1, **to(lax.rem(here + k, sections), depth))
    for k in range(1, copies):
        pl.semaphore_signal(barrier, inc=1, **to(here, lax.rem(depth + k, copies)))

    def point_send(kind, source, target, distance):
        return pltpu.make_async_remote_copy(
            src_ref=source, dst_ref=target,
            send_sem=send_point.at[kind], recv_sem=take_point.at[kind],
            **to(lax.rem(here + distance, sections), depth),
        )

    give_relaxed = point_send(0, relaxed, left_relaxed, 1)
    give_far_relaxed = point_send(1, relaxed, far_relaxed, half)
    give_middle = point_send(2, middle, left_middle, 1)
    give_final = point_send(3, final, left_final, 1)
    give_far_final = point_send(4, final, far_final, half)

    def state_send(slot, target, distance, row):
        return pltpu.make_async_remote_copy(
            src_ref=states.at[slot], dst_ref=target.at[slot],
            send_sem=send_state.at[row, slot], recv_sem=take_state.at[row, slot],
            **to(lax.rem(here + distance, sections), depth),
        )

    def give_left(slot):
        return state_send(slot, lefts, 1, 0)

    def give_far(slot):
        return state_send(slot, fars, half, 1)

    def across_copy(k):
        return pltpu.make_async_remote_copy(
            src_ref=tile, dst_ref=across.at[depth],
            send_sem=across_send.at[k - 1], recv_sem=across_take.at[k - 1],
            **to(here, lax.rem(depth + k, copies)),
        )

    def along_copy(k):
        return pltpu.make_async_remote_copy(
            src_ref=summed, dst_ref=along.at[k - 1],
            send_sem=along_send.at[k - 1], recv_sem=along_take.at[k - 1],
            **to(lax.rem(here + k, sections), depth),
        )

    def normalise(part, values, slot):
        mean_square = jnp.mean(values * values, axis=-1, keepdims=True)
        normed[part * rows : (part + 1) * rows, :] = (
            values * lax.rsqrt(mean_square + epsilon) * gain[pl.ds(slot, 1), :]
        ).astype(jnp.bfloat16)

    def project_in(parts, slot):
        step = ff // 4
        for i in range(4):
            cols = slice(i * step, (i + 1) * step)
            hidden[: parts * rows, cols] = jax.nn.gelu(
                jnp.dot(
                    normed[: parts * rows, :], w_in[slot, :, cols],
                    preferred_element_type=jnp.float32,
                ),
                approximate=True,
            ).astype(jnp.bfloat16)

    def project_out(parts, slot):
        step = width // 4
        for i in range(4):
            cols = slice(i * step, (i + 1) * step)
            total[: parts * rows, cols] = jnp.dot(
                hidden[: parts * rows, :], w_out[slot, :, cols],
                preferred_element_type=jnp.float32,
            )

    def update(part):
        return total[part * rows : (part + 1) * rows, :]

    load_start.wait()
    load_gain.wait()
    cur[...] = start[...]

    def first_pass(slot, carry):
        normalise(0, cur[...], slot)
        normalise(1, start[...], slot)
        load_first(slot).wait()

        @pl.when(slot + ahead < slot_count)
        def _():
            load_first(slot + ahead).start()

        project_in(2, slot)
        load_second(slot).wait()

        @pl.when(slot + ahead < slot_count)
        def _():
            load_second(slot + ahead).start()

        project_out(2, slot)
        state = cur[...] + update(0)
        cur[...] = state
        states[slot] = state
        return carry

    lax.fori_loop(0, slot_count, first_pass, 0)
    relaxed[...] = cur[...]
    pl.semaphore_wait(barrier, sections + copies - 2)

    @pl.when(here < end)
    def _():
        give_relaxed.start()

    @pl.when(here == half - 1)
    def _():
        give_far_relaxed.start()

    @pl.when(here == half - 1)
    def _():
        wide_start[...] = start[...] + 16.0 * update(1)

    @pl.when(here == 0)
    def _():
        final[...] = relaxed[...]
        give_far_final.start()
        for slot in range(slot_last):
            give_left(slot).start()
            give_far(slot).start()
            four[slot] = jnp.zeros_like(start)
        four[slot_last] = relaxed[...] - (start[...] + 4.0 * update(1))
        tile[...] = jnp.zeros_like(tile)

    @pl.when(here > 0)
    def _():
        give_relaxed.wait_recv()
        cur[...] = left_relaxed[...]

        def second_pass(slot, carry):
            normalise(0, cur[...], slot)

            @pl.when(slot == slot_last)
            def _():
                normalise(1, left_relaxed[...], slot)

            project_in(2, slot)
            project_out(2, slot)
            state = cur[...] + update(0)
            cur[...] = state
            states[slot] = state
            return carry

        lax.fori_loop(0, slot_count, second_pass, 0)

        @pl.when(here == 1)
        def _():
            final[...] = cur[...]
            give_final.start()
            give_far_final.start()
            for slot in range(slot_last):
                give_left(slot).start()
                give_far(slot).start()

        @pl.when(here == half)
        def _():
            middle[...] = cur[...]
            give_middle.start()

        point = cur[...]
        source = point - (left_relaxed[...] + 4.0 * update(1))
        rhs[...] = source
        fine[...] = point
        near[...] = update(0)

        @pl.when(here == 1)
        def _():
            four[slot_last] = source

    def take_sums():
        gap = fine[...] - relaxed[...]
        near_term = near[...]
        lane = lax.broadcasted_iota(jnp.int32, tile.shape, 1) == here - 1
        row = lax.broadcasted_iota(jnp.int32, tile.shape, 0)
        tile[...] = jnp.where(lane & (row == 0), jnp.sum(gap * gap), 0.0) + jnp.where(
            lane & (row == 1), jnp.sum(near_term * near_term), 0.0
        )

    def coarse_pass(r, carry):
        middle_round = (r == 0) & (here > half)
        wide_round = (r == 1) & (here == end)
        final_round = (r == 2) & (here > 1)

        @pl.when(middle_round | wide_round | final_round)
        def _():
            @pl.when(middle_round)
            def _():
                give_middle.wait_recv()
                normalise(0, left_middle[...], slot_last)

            @pl.when(wide_round)
            def _():
                give_far_relaxed.wait_recv()
                normalise(1, far_relaxed[...], slot_last)
                give_far_final.wait_recv()
                normalise(0, far_final[...], slot_last)

            @pl.when(final_round)
            def _():
                @pl.when((here >= half) & (here < end))
                def _():
                    give_far_final.wait_recv()
                    normalise(1, far_final[...], slot_last)

                give_final.wait_recv()
                normalise(0, left_final[...], slot_last)

            project_in(2, slot_last)
            project_out(2, slot_last)

            @pl.when(middle_round)
            def _():
                middle[...] = left_middle[...] + 4.0 * update(0) + rhs[...]

                @pl.when(here < end)
                def _():
                    give_middle.start()

            @pl.when(wide_round)
            def _():
                stepped = far_final[...] + 16.0 * update(0)
                point = stepped + (middle[...] - (far_relaxed[...] + 16.0 * update(1)))
                final[...] = point
                sixteen[slot_last] = point - stepped

            @pl.when(final_round)
            def _():
                stepped = left_final[...] + 4.0 * update(0)

                @pl.when(here < end)
                def _():
                    final[...] = stepped + rhs[...]
                    give_final.start()

                @pl.when(here < half)
                def _():
                    give_far_final.start()

                point = final[...]
                four[slot_last] = point - stepped

                @pl.when(here == half - 1)
                def _():
                    sixteen[slot_last] = point - wide_start[...]

                @pl.when((here >= half) & (here < end))
                def _():
                    sixteen[slot_last] = point - (far_final[...] + 16.0 * update(1))

        @pl.when(r == 0)
        def _():
            @pl.when(here > 0)
            def _():
                take_sums()

            across[depth] = tile[...]
            for k in range(1, copies):
                across_copy(k).start()

        return carry

    lax.fori_loop(0, 3, coarse_pass, 0)

    states[slot_last] = final[...]

    def advance(slot):
        state = cur[...] + update(0)
        cur[...] = state
        states[slot] = state

        @pl.when(here < end)
        def _():
            give_left(slot).start()

        @pl.when(here < half)
        def _():
            give_far(slot).start()

    def take_left(slot, part):
        give_left(slot).wait_recv()
        normalise(part, lefts[slot], slot)

    def take_far(slot, part):
        give_far(slot).wait_recv()
        normalise(part, fars[slot], slot)

    def defect_four(slot, part):
        four[slot] = states[slot] - (lefts[slot] + 4.0 * update(part))

    def defect_sixteen(slot, part):
        sixteen[slot] = states[slot] - (fars[slot] + 16.0 * update(part))

    @pl.when((here > 1) & (here < end))
    def _():
        cur[...] = left_final[...]

        def state_pass(slot, carry):
            normalise(0, cur[...], slot)
            project_in(2, slot)
            project_out(2, slot)
            advance(slot)
            return carry

        lax.fori_loop(0, slot_last, state_pass, 0)

    for k in range(1, copies):
        across_copy(k).wait()
    gathered = across[0]
    for k in range(1, copies):
        gathered = gathered + across[k]
    summed[...] = gathered
    for k in range(1, sections):
        along_copy(k).start()

    @pl.when((here > 0) & (here < end))
    def _():
        def defect_pass(slot, carry):
            take_left(slot, 0)

            @pl.when(here >= half)
            def _():
                take_far(slot, 1)

            project_in(2, slot)
            project_out(2, slot)
            defect_four(slot, 0)

            @pl.when(here >= half)
            def _():
                defect_sixteen(slot, 1)

            return carry

        lax.fori_loop(0, slot_last, defect_pass, 0)

    @pl.when(here == end)
    def _():
        cur[...] = left_final[...]

        def last_pass(slot, carry):
            normalise(0, cur[...], slot)
            take_far(slot, 2)
            take_left(slot, 1)
            project_in(3, slot)
            project_out(3, slot)
            state = cur[...] + update(0)
            cur[...] = state
            states[slot] = state
            defect_four(slot, 1)
            defect_sixteen(slot, 2)
            return carry

        lax.fori_loop(0, slot_last, last_pass, 0)

    @pl.when(here < half)
    def _():
        for slot in range(slot_last):
            sixteen[slot] = jnp.zeros_like(start)

    @pl.when(here < half - 1)
    def _():
        sixteen[slot_last] = jnp.zeros_like(start)

    @pl.when(here < end)
    def _():
        give_relaxed.wait_send()
        for slot in range(slot_last):
            give_left(slot).wait_send()

    @pl.when(here == half - 1)
    def _():
        give_far_relaxed.wait_send()

    @pl.when((here >= half) & (here < end))
    def _():
        give_middle.wait_send()

    @pl.when((here > 0) & (here < end))
    def _():
        give_final.wait_send()

    @pl.when(here < half)
    def _():
        give_far_final.wait_send()
        for slot in range(slot_last):
            give_far(slot).wait_send()

    sums = summed[...]
    for k in range(1, sections):
        along_copy(k).wait()
        sums = sums + along[k - 1]
    ratios[...] = jnp.sqrt(sums[0:1] / (sums[1:2] + epsilon))


def finish_kernel(states, ratios, four, sixteen, out_states, out_ratios, out_four, out_sixteen, store):
    pairs = ((states, out_states), (four, out_four), (sixteen, out_sixteen))
    copies = [
        pltpu.make_async_copy(held, out, store.at[i]) for i, (held, out) in enumerate(pairs)
    ]
    for copy in copies:
        copy.start()
    out_ratios[...] = ratios[0, : out_ratios.shape[0]]
    for copy in copies:
        copy.wait()


def cycle(initial, norm_gains, first_weights, second_weights):
    sections = lax.axis_size("layer")
    copies = lax.axis_size("dp")
    shape = initial.shape
    slot_count, width, ff = first_weights.shape
    rows = shape[0]
    anywhere = pl.BlockSpec(memory_space=pl.ANY)
    inside = pl.BlockSpec(memory_space=pltpu.VMEM)
    held = (slot_count,) + shape
    inner = (slot_count - 1,) + shape
    dma = pltpu.SemaphoreType.DMA

    def single(*dims):
        return pltpu.VMEM(dims, jnp.float32)

    states, four, sixteen, ratios = pl.pallas_call(
        lambda *refs: cycle_kernel(sections, copies, *refs),
        out_shape=(
            pltpu.VMEM(held, jnp.float32),
            pltpu.VMEM(held, jnp.float32),
            pltpu.VMEM(held, jnp.float32),
            pltpu.VMEM((1, 128), jnp.float32),
        ),
        in_specs=[pl.BlockSpec(memory_space=pltpu.HBM)] * 4,
        out_specs=(inside,) * 4,
        scratch_shapes=[
            pltpu.VMEM(first_weights.shape, jnp.bfloat16),
            pltpu.VMEM(second_weights.shape, jnp.bfloat16),
            single(slot_count, width),
            single(*shape),
            pltpu.VMEM((3 * rows, width), jnp.bfloat16),
            pltpu.VMEM((3 * rows, ff), jnp.bfloat16),
            single(3 * rows, width),
            single(*shape),
            single(*shape), single(*shape), single(*shape), single(*shape), single(*shape), single(*shape),
            single(*shape), single(*shape), single(*shape), single(*shape), single(*shape), single(*shape),
            single(*inner), single(*inner),
            single(8, 128), single(copies, 8, 128), single(sections - 1, 8, 128), single(8, 128),
            dma((slot_count,)), dma((slot_count,)), dma((2,)),
            dma((5,)), dma((5,)), dma((2, slot_count - 1)), dma((2, slot_count - 1)),
            dma((copies - 1,)), dma((copies - 1,)),
            dma((sections - 1,)), dma((sections - 1,)),
        ],
        compiler_params=pltpu.CompilerParams(
            collective_id=0, has_side_effects=True, vmem_limit_bytes=62384 * 1024
        ),
        name="cycle",
    )(initial, norm_gains, first_weights, second_weights)
    out_states, out_ratios, out_four, out_sixteen = pl.pallas_call(
        finish_kernel,
        out_shape=(
            jax.ShapeDtypeStruct(held, jnp.float32),
            jax.ShapeDtypeStruct((sections - 1,), jnp.float32),
            jax.ShapeDtypeStruct(held, jnp.float32),
            jax.ShapeDtypeStruct(held, jnp.float32),
        ),
        in_specs=[inside] * 4,
        out_specs=(anywhere, inside, anywhere, anywhere),
        scratch_shapes=[dma((3,))],
        compiler_params=pltpu.CompilerParams(vmem_limit_bytes=8 * 1024 * 1024),
        name="finish",
    )(states, ratios, four, sixteen)
    return (out_states, out_ratios, out_four, out_sixteen)


def chosen(initial, norm_gains, first_weights, second_weights):
    sections = lax.axis_size("layer")
    fits = first_weights.shape[0] == 4 and sections == 8 and lax.axis_size("dp") > 1
    return (cycle if fits else local)(initial, norm_gains, first_weights, second_weights)


def solution(mesh):
    placed = (P("dp", None), P("layer", None), P("layer", None, None), P("layer", None, None))
    return jax.shard_map(
        chosen,
        mesh=mesh,
        in_specs=placed,
        out_specs=(P("layer", "dp", None), P(), P("layer", "dp", None), P("layer", "dp", None)),
        check_vma=False,
    )
```

```python
import jax
import jax.numpy as jnp
from jax import lax
from jax.experimental import pallas as pl
from jax.experimental.pallas import tpu as pltpu
from jax.sharding import PartitionSpec as P

epsilon = 1e-06


def shifted(block, axis, distance):
    devices = range(lax.axis_size(axis))
    route = [(i - distance, i) for i in devices if i - distance in devices]
    return lax.ppermute(block, axis, route)


def branch(row_block, weight_in, weight_out, gain_row):
    mean_square = jnp.mean(row_block * row_block, axis=-1, keepdims=True)
    normed = (row_block * lax.rsqrt(mean_square + epsilon) * gain_row).astype(jnp.bfloat16)
    hidden = jax.nn.gelu(
        jnp.dot(normed, weight_in, preferred_element_type=jnp.float32), approximate=True
    ).astype(jnp.bfloat16)
    return jnp.dot(hidden, weight_out, preferred_element_type=jnp.float32)


def local(initial, norm_gains, first_weights, second_weights):
    slot_count = first_weights.shape[0]
    sections = lax.axis_size("layer")
    layer_total = slot_count * sections
    norm_count = layer_total // 4 - 1
    first_point = lax.axis_index("layer") * slot_count
    points = first_point + jnp.arange(slot_count, dtype=jnp.int32) + 1
    spacings = (1, 4, 16)

    def shaped(flags, rank):
        return flags.reshape((slot_count,) + (1,) * (rank - 1))

    def previous(values, level_index):
        spacing = spacings[level_index]
        if spacing >= slot_count:
            portion = values
            distance = spacing // slot_count
        else:
            portion = values[slot_count - spacing :]
            distance = 1
        if level_index == 0:
            arrived = shifted(portion, "layer", distance)
        elif level_index == 1:
            arrived = shifted(portion, "layer", distance)
        else:
            arrived = shifted(portion, "layer", distance)
        if spacing < slot_count:
            arrived = jnp.concatenate([arrived, values[: slot_count - spacing]], axis=0)
        return arrived

    def incoming(values, level_index, anchor):
        arrived = previous(values, level_index)
        from_anchor = shaped(points - spacings[level_index] == 0, values.ndim)
        return jnp.where(from_anchor, anchor, arrived)

    def advance(before, level_index, active, right_side):
        factor = float(spacings[level_index])
        results = []
        for slot in range(slot_count):

            def advance_compute(values, source, slot=slot):
                return (
                    values
                    + factor
                    * branch(values, first_weights[slot], second_weights[slot], norm_gains[slot])
                    + source
                )

            def advance_unchanged(values, source):
                return values

            source = right_side[slot] if right_side is not None else jnp.zeros_like(before[slot])
            results.append(
                lax.cond(active[slot], advance_compute, advance_unchanged, before[slot], source)
            )
        return jnp.stack(results)

    def relaxation(current, level_index, residues, right_side, anchor):
        modulus = 4 * spacings[level_index]
        for residue in residues:
            before = incoming(current, level_index, anchor)
            active = points % modulus == residue
            current = jnp.where(
                shaped(active, 3), advance(before, level_index, active, right_side), current
            )
        return (current, None)

    def restrict(current, level_index, right_side, anchor):
        spacing = spacings[level_index]
        factor = float(spacing)
        wide_factor = float(4 * spacing)
        before = incoming(current, level_index, anchor)
        far_state = incoming(current, level_index + 1, anchor)
        active = points % (4 * spacing) == 0
        row_count = current.shape[1]
        coarse_list = []
        gap_list = []
        step_list = []
        for slot in range(slot_count):

            def restrict_compute(near, distant, held, source, slot=slot):
                update = branch(
                    jnp.concatenate([near, distant], axis=0),
                    first_weights[slot],
                    second_weights[slot],
                    norm_gains[slot],
                )
                near_term = update[:row_count]
                fine_value = near + factor * near_term + source
                coarse = fine_value - (distant + wide_factor * update[row_count:])
                gap = fine_value - held
                return (coarse, jnp.sum(gap * gap), jnp.sum(near_term * near_term))

            def restrict_unchanged(near, distant, held, source):
                nothing = jnp.zeros((), near.dtype)
                return (jnp.zeros_like(near), nothing, nothing)

            source = right_side[slot] if right_side is not None else jnp.zeros_like(before[slot])
            coarse, gap_sum, step_sum = lax.cond(
                active[slot],
                restrict_compute,
                restrict_unchanged,
                before[slot],
                far_state[slot],
                current[slot],
                source,
            )
            coarse_list.append(coarse)
            gap_list.append(gap_sum)
            step_list.append(step_sum)
        return (jnp.stack(coarse_list), jnp.stack(gap_list), jnp.stack(step_list))

    def defects(current, level_index, anchor):
        spacing = spacings[level_index]
        factor = float(spacing)
        before = incoming(current, level_index, anchor)
        stepped = []
        for slot in range(slot_count):
            stepped.append(
                before[slot]
                + factor
                * branch(before[slot], first_weights[slot], second_weights[slot], norm_gains[slot])
            )
        valid = shaped(points >= spacing, 3)
        return jnp.where(valid, current - jnp.stack(stepped), 0.0)

    def multigrid_cycle(anchor):
        current = jnp.broadcast_to(anchor, (slot_count,) + anchor.shape)
        current, unused = relaxation(current, 0, (1, 2, 3), None, anchor)
        current, unused = relaxation(current, 0, (0,), None, anchor)
        current, carried = relaxation(current, 0, (1, 2, 3), None, anchor)
        rhs_one, gap_sums, step_sums = restrict(current, 0, None, anchor)
        current, carried = relaxation(current, 1, (4, 8, 12), rhs_one, anchor)
        rhs_two, unused_gaps, unused_steps = restrict(current, 1, rhs_one, anchor)
        for coarse_step in range(1, layer_total // 16 + 1):
            active = points == 16 * coarse_step
            before = incoming(current, 2, anchor)
            current = jnp.where(shaped(active, 3), advance(before, 2, active, rhs_two), current)
        current, unused = relaxation(current, 1, (4, 8, 12), rhs_one, anchor)
        current, unused = relaxation(current, 0, (1, 2, 3), None, anchor)
        defects_four = defects(current, 1, anchor)
        defects_sixteen = defects(current, 2, anchor)
        return (current, gap_sums, step_sums, defects_four, defects_sixteen)

    portions = [initial]
    outcomes = [multigrid_cycle(portion) for portion in portions]
    layer_states = jnp.concatenate([outcome[0] for outcome in outcomes], axis=1)
    defects_four = jnp.concatenate([outcome[3] for outcome in outcomes], axis=1)
    defects_sixteen = jnp.concatenate([outcome[4] for outcome in outcomes], axis=1)
    gap_sums = outcomes[0][1]
    step_sums = outcomes[0][2]
    counted = (points % 4 == 0) & (points >= 8)
    entry_index = points // 4 - 2
    one_hot = (
        (jnp.arange(norm_count, dtype=jnp.int32)[None, :] == entry_index[:, None])
        & counted[:, None]
    ).astype(jnp.float32)
    gap_vector = jnp.sum(gap_sums[:, None] * one_hot, axis=0)
    step_vector = jnp.sum(step_sums[:, None] * one_hot, axis=0)
    gap_total, step_total = lax.psum((gap_vector, step_vector), ("layer", "dp"))
    residual_ratios = jnp.sqrt(gap_total / (step_total + epsilon))
    return (layer_states, residual_ratios, defects_four, defects_sixteen)


def cycle_kernel(
    sections, copies,
    initial, norm_gains, first_weights, second_weights,
    states, four, sixteen, ratios,
    w_in, w_out, gain, start, normed, hidden, total, cur,
    relaxed, middle, final, rhs, wide_start,
    fine, near, left_relaxed, left_middle, left_final, far_relaxed, far_final, lefts, fars,
    scale, partial, tile, across, along, summed,
    load_in, load_out, load_small,
    send_point, take_point, send_state, take_state,
    across_send, across_take, along_send, along_take,
):
    here = lax.axis_index("layer")
    depth = lax.axis_index("dp")
    slot_count, width, ff = w_in.shape
    rows = start.shape[0]
    half = sections // 2
    end = sections - 1
    slot_last = slot_count - 1

    def to(layer, dp):
        return dict(device_id=(layer, dp), device_id_type=pl.DeviceIdType.MESH)

    def load_first(slot):
        return pltpu.make_async_copy(first_weights.at[slot], w_in.at[slot], load_in.at[slot])

    def load_second(slot):
        return pltpu.make_async_copy(second_weights.at[slot], w_out.at[slot], load_out.at[slot])

    load_start = pltpu.make_async_copy(initial, start, load_small.at[0])
    load_gain = pltpu.make_async_copy(norm_gains, gain, load_small.at[1])
    load_start.start()
    load_gain.start()
    ahead = min(2, slot_count)
    for slot in range(ahead):
        load_first(slot).start()
        load_second(slot).start()

    barrier = pltpu.get_barrier_semaphore()
    for k in range(1, sections):
        pl.semaphore_signal(barrier, inc=1, **to(lax.rem(here + k, sections), depth))
    for k in range(1, copies):
        pl.semaphore_signal(barrier, inc=1, **to(here, lax.rem(depth + k, copies)))

    def point_send(kind, source, target, distance):
        return pltpu.make_async_remote_copy(
            src_ref=source, dst_ref=target,
            send_sem=send_point.at[kind], recv_sem=take_point.at[kind],
            **to(lax.rem(here + distance, sections), depth),
        )

    give_relaxed = point_send(0, relaxed, left_relaxed, 1)
    give_far_relaxed = point_send(1, relaxed, far_relaxed, half)
    give_far_final = point_send(2, final, far_final, half)
    parts_of_row = [pl.ds(i * width // 2, width // 2) for i in range(2)]
    give_middle = [
        point_send(3 + i, middle.at[:, cols], left_middle.at[:, cols], 1)
        for i, cols in enumerate(parts_of_row)
    ]
    give_final = [
        point_send(5 + i, final.at[:, cols], left_final.at[:, cols], 1)
        for i, cols in enumerate(parts_of_row)
    ]

    def state_send(slot, target, distance, row):
        return pltpu.make_async_remote_copy(
            src_ref=states.at[slot], dst_ref=target.at[slot],
            send_sem=send_state.at[row, slot], recv_sem=take_state.at[row, slot],
            **to(lax.rem(here + distance, sections), depth),
        )

    def give_left(slot):
        return state_send(slot, lefts, 1, 0)

    def give_far(slot):
        return state_send(slot, fars, half, 1)

    def across_copy(k):
        return pltpu.make_async_remote_copy(
            src_ref=tile, dst_ref=across.at[depth],
            send_sem=across_send.at[k - 1], recv_sem=across_take.at[k - 1],
            **to(here, lax.rem(depth + k, copies)),
        )

    def along_copy(k):
        return pltpu.make_async_remote_copy(
            src_ref=summed, dst_ref=along.at[k - 1],
            send_sem=along_send.at[k - 1], recv_sem=along_take.at[k - 1],
            **to(lax.rem(here + k, sections), depth),
        )

    def normalise(part, values, slot):
        mean_square = jnp.mean(values * values, axis=-1, keepdims=True)
        normed[part * rows : (part + 1) * rows, :] = (
            values * lax.rsqrt(mean_square + epsilon) * gain[pl.ds(slot, 1), :]
        ).astype(jnp.bfloat16)

    def project_in(parts, slot):
        step = ff // 4
        for i in range(4):
            cols = slice(i * step, (i + 1) * step)
            hidden[: parts * rows, cols] = jax.nn.gelu(
                jnp.dot(
                    normed[: parts * rows, :], w_in[slot, :, cols],
                    preferred_element_type=jnp.float32,
                ),
                approximate=True,
            ).astype(jnp.bfloat16)

    def project_out(parts, slot):
        step = width // 4
        for i in range(4):
            cols = slice(i * step, (i + 1) * step)
            total[: parts * rows, cols] = jnp.dot(
                hidden[: parts * rows, :], w_out[slot, :, cols],
                preferred_element_type=jnp.float32,
            )

    def update(part):
        return total[part * rows : (part + 1) * rows, :]

    load_start.wait()
    load_gain.wait()
    cur[...] = start[...]

    def first_pass(slot, carry):
        normalise(0, cur[...], slot)
        normalise(1, start[...], slot)
        load_first(slot).wait()

        @pl.when(slot + ahead < slot_count)
        def _():
            load_first(slot + ahead).start()

        project_in(2, slot)
        load_second(slot).wait()

        @pl.when(slot + ahead < slot_count)
        def _():
            load_second(slot + ahead).start()

        project_out(2, slot)
        state = cur[...] + update(0)
        cur[...] = state
        states[slot] = state
        return carry

    lax.fori_loop(0, slot_count, first_pass, 0)
    relaxed[...] = cur[...]
    pl.semaphore_wait(barrier, sections + copies - 2)

    @pl.when(here < end)
    def _():
        give_relaxed.start()

    @pl.when(here == half - 1)
    def _():
        give_far_relaxed.start()

    @pl.when(here == half - 1)
    def _():
        wide_start[...] = start[...] + 16.0 * update(1)

    @pl.when(here == 0)
    def _():
        final[...] = relaxed[...]
        give_far_final.start()
        for slot in range(slot_last):
            give_left(slot).start()
            give_far(slot).start()
            four[slot] = jnp.zeros_like(start)
        four[slot_last] = relaxed[...] - (start[...] + 4.0 * update(1))
        tile[...] = jnp.zeros_like(tile)

    @pl.when(here > 0)
    def _():
        give_relaxed.wait_recv()
        cur[...] = left_relaxed[...]

        def second_pass(slot, carry):
            normalise(0, cur[...], slot)

            @pl.when(slot == slot_last)
            def _():
                normalise(1, left_relaxed[...], slot)

            project_in(2, slot)
            project_out(2, slot)
            state = cur[...] + update(0)
            cur[...] = state
            states[slot] = state
            return carry

        lax.fori_loop(0, slot_count, second_pass, 0)

        @pl.when(here == 1)
        def _():
            final[...] = cur[...]
            for copy in give_final:
                copy.start()
            give_far_final.start()
            for slot in range(slot_last):
                give_left(slot).start()
                give_far(slot).start()

        @pl.when(here == half)
        def _():
            middle[...] = cur[...]
            for copy in give_middle:
                copy.start()

        point = cur[...]
        source = point - (left_relaxed[...] + 4.0 * update(1))
        rhs[...] = source
        fine[...] = point
        near[...] = update(0)

        @pl.when(here == 1)
        def _():
            four[slot_last] = source

    def take_sums():
        gap = fine[...] - relaxed[...]
        near_term = near[...]
        lane = lax.broadcasted_iota(jnp.int32, tile.shape, 1) == here - 1
        row = lax.broadcasted_iota(jnp.int32, tile.shape, 0)
        tile[...] = jnp.where(lane & (row == 0), jnp.sum(gap * gap), 0.0) + jnp.where(
            lane & (row == 1), jnp.sum(near_term * near_term), 0.0
        )

    halves = [slice(i * width // 2, (i + 1) * width // 2) for i in range(2)]

    def weigh(part, source):
        values = source[...]
        span = slice(part * rows, (part + 1) * rows)
        mean_square = jnp.mean(values * values, axis=-1, keepdims=True)
        normed[span, :] = (values * gain[slot_last : slot_last + 1, :]).astype(jnp.bfloat16)
        scale[span, :] = jnp.broadcast_to(lax.rsqrt(mean_square + epsilon), (rows, 128))

    def weigh_half(i, source):
        cols = halves[i]
        values = source[:, cols]
        squares = jnp.sum(values * values, axis=-1, keepdims=True)
        normed[:rows, cols] = (values * gain[slot_last : slot_last + 1, cols]).astype(jnp.bfloat16)
        if i == 0:
            scale[:rows, :] = jnp.broadcast_to(squares, (rows, 128))
        else:
            scale[:rows, :] = lax.rsqrt((scale[:rows, :] + squares) * (1.0 / width) + epsilon)

    def project_half(i):
        step = ff // 4
        for j in range(4):
            cols = slice(j * step, (j + 1) * step)
            product = jnp.dot(
                normed[: 2 * rows, halves[i]], w_in[slot_last, halves[i], cols],
                preferred_element_type=jnp.float32,
            )
            if i == 0:
                partial[:, cols] = product
            else:
                hidden[: 2 * rows, cols] = jax.nn.gelu(
                    (partial[:, cols] + product) * scale[:, 0:1], approximate=True
                ).astype(jnp.bfloat16)

    def project_out_half(i):
        step = width // 4
        for j in (2 * i, 2 * i + 1):
            cols = slice(j * step, (j + 1) * step)
            total[: 2 * rows, cols] = jnp.dot(
                hidden[: 2 * rows, :], w_out[slot_last, :, cols],
                preferred_element_type=jnp.float32,
            )

    def exchange():
        for k in range(1, copies):
            across_copy(k).wait()
        gathered = across[0]
        for k in range(1, copies):
            gathered = gathered + across[k]
        summed[...] = gathered
        for k in range(1, sections):
            along_copy(k).start()

    def coarse_pass(r, carry):
        middle_round = (r == 0) & (here > half)
        wide_round = (r == 1) & (here == end)
        final_round = (r == 2) & (here > 1)

        @pl.when(middle_round | wide_round | final_round)
        def _():
            @pl.when(wide_round)
            def _():
                give_far_relaxed.wait_recv()
                weigh(1, far_relaxed)
                give_far_final.wait_recv()

            @pl.when(final_round & (here >= half) & (here < end))
            def _():
                give_far_final.wait_recv()
                weigh(1, far_final)

            for i in range(2):
                @pl.when(middle_round)
                def _(i=i):
                    give_middle[i].wait_recv()
                    weigh_half(i, left_middle)

                @pl.when(wide_round)
                def _(i=i):
                    weigh_half(i, far_final)

                @pl.when(final_round)
                def _(i=i):
                    give_final[i].wait_recv()
                    weigh_half(i, left_final)

                project_half(i)

            for i in range(2):
                project_out_half(i)
                cols = halves[i]

                @pl.when(middle_round)
                def _(i=i, cols=cols):
                    middle[:, cols] = left_middle[:, cols] + 4.0 * total[:rows, cols] + rhs[:, cols]

                    @pl.when(here < end)
                    def _():
                        give_middle[i].start()

                @pl.when(final_round & (here < end))
                def _(i=i, cols=cols):
                    final[:, cols] = left_final[:, cols] + 4.0 * total[:rows, cols] + rhs[:, cols]
                    give_final[i].start()

            @pl.when(wide_round)
            def _():
                stepped = far_final[...] + 16.0 * update(0)
                point = stepped + (middle[...] - (far_relaxed[...] + 16.0 * update(1)))
                final[...] = point
                sixteen[slot_last] = point - stepped

            @pl.when(final_round)
            def _():
                @pl.when(here < half)
                def _():
                    give_far_final.start()

                point = final[...]
                four[slot_last] = point - (left_final[...] + 4.0 * update(0))

                @pl.when(here == half - 1)
                def _():
                    sixteen[slot_last] = point - wide_start[...]

                @pl.when((here >= half) & (here < end))
                def _():
                    sixteen[slot_last] = point - (far_final[...] + 16.0 * update(1))

        @pl.when(r == 0)
        def _():
            @pl.when(here > 0)
            def _():
                take_sums()

            across[depth] = tile[...]
            for k in range(1, copies):
                across_copy(k).start()

        @pl.when((r == 1) & ((here < 2) | (here >= half)))
        def _():
            exchange()

        return carry

    lax.fori_loop(0, 3, coarse_pass, 0)

    states[slot_last] = final[...]

    def advance(slot):
        state = cur[...] + update(0)
        cur[...] = state
        states[slot] = state

        @pl.when(here < end)
        def _():
            give_left(slot).start()

        @pl.when(here < half)
        def _():
            give_far(slot).start()

    def take_left(slot, part):
        give_left(slot).wait_recv()
        normalise(part, lefts[slot], slot)

    def take_far(slot, part):
        give_far(slot).wait_recv()
        normalise(part, fars[slot], slot)

    def defect_four(slot, part):
        four[slot] = states[slot] - (lefts[slot] + 4.0 * update(part))

    def defect_sixteen(slot, part):
        sixteen[slot] = states[slot] - (fars[slot] + 16.0 * update(part))

    @pl.when((here > 1) & (here < end))
    def _():
        cur[...] = left_final[...]

        def state_pass(slot, carry):
            normalise(0, cur[...], slot)
            project_in(2, slot)
            project_out(2, slot)
            advance(slot)
            return carry

        lax.fori_loop(0, slot_last, state_pass, 0)

    @pl.when((here > 1) & (here < half))
    def _():
        exchange()

    @pl.when((here > 0) & (here < end))
    def _():
        def defect_pass(slot, carry):
            take_left(slot, 0)

            @pl.when(here >= half)
            def _():
                take_far(slot, 1)

            project_in(2, slot)
            project_out(2, slot)
            defect_four(slot, 0)

            @pl.when(here >= half)
            def _():
                defect_sixteen(slot, 1)

            return carry

        lax.fori_loop(0, slot_last, defect_pass, 0)

    @pl.when(here == end)
    def _():
        cur[...] = left_final[...]

        def last_pass(slot, carry):
            normalise(0, cur[...], slot)
            take_far(slot, 2)
            take_left(slot, 1)
            project_in(3, slot)
            project_out(3, slot)
            state = cur[...] + update(0)
            cur[...] = state
            states[slot] = state
            defect_four(slot, 1)
            defect_sixteen(slot, 2)
            return carry

        lax.fori_loop(0, slot_last, last_pass, 0)

    @pl.when(here < half)
    def _():
        for slot in range(slot_last):
            sixteen[slot] = jnp.zeros_like(start)

    @pl.when(here < half - 1)
    def _():
        sixteen[slot_last] = jnp.zeros_like(start)

    @pl.when(here < end)
    def _():
        give_relaxed.wait_send()
        for slot in range(slot_last):
            give_left(slot).wait_send()

    @pl.when(here == half - 1)
    def _():
        give_far_relaxed.wait_send()

    @pl.when((here >= half) & (here < end))
    def _():
        for copy in give_middle:
            copy.wait_send()

    @pl.when((here > 0) & (here < end))
    def _():
        for copy in give_final:
            copy.wait_send()

    @pl.when(here < half)
    def _():
        give_far_final.wait_send()
        for slot in range(slot_last):
            give_far(slot).wait_send()

    sums = summed[...]
    for k in range(1, sections):
        along_copy(k).wait()
        sums = sums + along[k - 1]
    ratios[...] = jnp.sqrt(sums[0:1] / (sums[1:2] + epsilon))


def finish_kernel(states, ratios, four, sixteen, out_states, out_ratios, out_four, out_sixteen, store):
    pairs = ((states, out_states), (four, out_four), (sixteen, out_sixteen))
    copies = [
        pltpu.make_async_copy(held, out, store.at[i]) for i, (held, out) in enumerate(pairs)
    ]
    for copy in copies:
        copy.start()
    out_ratios[...] = ratios[0, : out_ratios.shape[0]]
    for copy in copies:
        copy.wait()


def cycle(initial, norm_gains, first_weights, second_weights):
    sections = lax.axis_size("layer")
    copies = lax.axis_size("dp")
    shape = initial.shape
    slot_count, width, ff = first_weights.shape
    rows = shape[0]
    anywhere = pl.BlockSpec(memory_space=pl.ANY)
    inside = pl.BlockSpec(memory_space=pltpu.VMEM)
    held = (slot_count,) + shape
    inner = (slot_count - 1,) + shape
    dma = pltpu.SemaphoreType.DMA

    def single(*dims):
        return pltpu.VMEM(dims, jnp.float32)

    states, four, sixteen, ratios = pl.pallas_call(
        lambda *refs: cycle_kernel(sections, copies, *refs),
        out_shape=(
            pltpu.VMEM(held, jnp.float32),
            pltpu.VMEM(held, jnp.float32),
            pltpu.VMEM(held, jnp.float32),
            pltpu.VMEM((1, 128), jnp.float32),
        ),
        in_specs=[pl.BlockSpec(memory_space=pltpu.HBM)] * 4,
        out_specs=(inside,) * 4,
        scratch_shapes=[
            pltpu.VMEM(first_weights.shape, jnp.bfloat16),
            pltpu.VMEM(second_weights.shape, jnp.bfloat16),
            single(slot_count, width),
            single(*shape),
            pltpu.VMEM((3 * rows, width), jnp.bfloat16),
            pltpu.VMEM((3 * rows, ff), jnp.bfloat16),
            single(3 * rows, width),
            single(*shape),
            single(*shape), single(*shape), single(*shape), single(*shape), single(*shape), single(*shape),
            single(*shape), single(*shape), single(*shape), single(*shape), single(*shape), single(*shape),
            single(*inner), single(*inner),
            single(2 * rows, 128), single(2 * rows, ff),
            single(8, 128), single(copies, 8, 128), single(sections - 1, 8, 128), single(8, 128),
            dma((slot_count,)), dma((slot_count,)), dma((2,)),
            dma((7,)), dma((7,)), dma((2, slot_count - 1)), dma((2, slot_count - 1)),
            dma((copies - 1,)), dma((copies - 1,)),
            dma((sections - 1,)), dma((sections - 1,)),
        ],
        compiler_params=pltpu.CompilerParams(
            collective_id=0, has_side_effects=True, vmem_limit_bytes=62384 * 1024
        ),
        name="cycle",
    )(initial, norm_gains, first_weights, second_weights)
    out_states, out_ratios, out_four, out_sixteen = pl.pallas_call(
        finish_kernel,
        out_shape=(
            jax.ShapeDtypeStruct(held, jnp.float32),
            jax.ShapeDtypeStruct((sections - 1,), jnp.float32),
            jax.ShapeDtypeStruct(held, jnp.float32),
            jax.ShapeDtypeStruct(held, jnp.float32),
        ),
        in_specs=[inside] * 4,
        out_specs=(anywhere, inside, anywhere, anywhere),
        scratch_shapes=[dma((3,))],
        compiler_params=pltpu.CompilerParams(vmem_limit_bytes=8 * 1024 * 1024),
        name="finish",
    )(states, ratios, four, sixteen)
    return (out_states, out_ratios, out_four, out_sixteen)


def chosen(initial, norm_gains, first_weights, second_weights):
    sections = lax.axis_size("layer")
    fits = first_weights.shape[0] == 4 and sections == 8 and lax.axis_size("dp") > 1
    return (cycle if fits else local)(initial, norm_gains, first_weights, second_weights)


def solution(mesh):
    placed = (P("dp", None), P("layer", None), P("layer", None, None), P("layer", None, None))
    return jax.shard_map(
        chosen,
        mesh=mesh,
        in_specs=placed,
        out_specs=(P("layer", "dp", None), P(), P("layer", "dp", None), P("layer", "dp", None)),
        check_vma=False,
    )
```
